8 devices in a mesh: sp: 8 (over z, y, x, core).
Axes of the slice: x: 2, y: 2, z: 1, core: 2. Of those that a mesh axis runs over, the one named last changes fastest.
Arguments:
- x: bfloat16 [8, 2048, 4096], P(None, 'sp')
- dy: bfloat16 [8, 2048, 4096], P(None, 'sp')
- prefix_len: int32 [8], replicated
- w_norm: bfloat16 [4096], replicated
- w_q: bfloat16 [4096, 4096], replicated
- w_k: bfloat16 [4096, 256], replicated
- w_v: bfloat16 [4096, 256], replicated
- w_o: bfloat16 [4096, 4096], replicated
Outputs:
- output 1: bfloat16 [8, 2048, 4096], P(None, 'sp')
- output 2: bfloat16 [8, 2048, 4096], P(None, 'sp')
- output 3: float32 [4096, 4096], replicated
- output 4: float32 [4096, 256], replicated
- output 5: float32 [4096, 256], replicated
- output 6: float32 [4096, 4096], replicated
- output 7: float32 [4096], replicated
All inputs are finite; a program needn't handle non-finite values.
Results may differ from the reference program's by a relative error of at most 0.0122329.
Values are sent between devices in bfloat16 or wider.
A program may use at most 1.25 GiB of HBM per device.

```python
import math
import functools
import jax
import jax.numpy as jnp
from jax import lax

BATCH = 8
SEQ_LEN = 2048
D_MODEL = 4096
HEADS = 16
HEAD_DIM = 256

ROPE_THETA = 10000.0
NORM_EPS = 1e-6
MASK_FILL = -1e30
ROW_BLOCK = math.gcd(SEQ_LEN, 256)


def setup_inputs(seed: int = 0) -> dict:
    keys = jax.random.split(jax.random.key(seed), 9)
    q_width = HEADS * HEAD_DIM
    x = jax.random.normal(keys[0], (BATCH, SEQ_LEN, D_MODEL), jnp.float32)
    dy = jax.random.normal(keys[1], (BATCH, SEQ_LEN, D_MODEL), jnp.float32)
    prefix_low = SEQ_LEN // 8
    prefix_high = 7 * SEQ_LEN // 8
    drawn_lens = jax.random.randint(keys[2], (BATCH,), prefix_low, prefix_high + 1, dtype=jnp.int32)
    drawn_lens = drawn_lens.at[0].set(prefix_low).at[1].set(prefix_high)
    prefix_len = jax.random.permutation(keys[3], drawn_lens)
    w_norm = 0.5 * jax.random.normal(keys[4], (D_MODEL,), jnp.float32)
    w_q = 1.2 * D_MODEL ** -0.5 * jax.random.normal(keys[5], (D_MODEL, q_width), jnp.float32)
    w_k = 1.2 * D_MODEL ** -0.5 * jax.random.normal(keys[6], (D_MODEL, HEAD_DIM), jnp.float32)
    w_v = D_MODEL ** -0.5 * jax.random.normal(keys[7], (D_MODEL, HEAD_DIM), jnp.float32)
    w_o = 2.0 * q_width ** -0.5 * jax.random.normal(keys[8], (q_width, D_MODEL), jnp.float32)
    return {'x': x.astype(jnp.bfloat16), 'dy': dy.astype(jnp.bfloat16), 'prefix_len': prefix_len, 'w_norm': w_norm.astype(jnp.bfloat16), 'w_q': w_q.astype(jnp.bfloat16), 'w_k': w_k.astype(jnp.bfloat16), 'w_v': w_v.astype(jnp.bfloat16), 'w_o': w_o.astype(jnp.bfloat16)}


def to_bf16_grid(values):
    return values.astype(jnp.bfloat16).astype(jnp.float32)


def rope_tables(positions):
    half = HEAD_DIM // 2
    frequencies = ROPE_THETA ** (-2.0 * jnp.arange(half, dtype=jnp.float32) / HEAD_DIM)
    angles = positions.astype(jnp.float32)[:, None] * frequencies[None, :]
    return jnp.cos(angles), jnp.sin(angles)


def apply_rope(vectors, cos_tab, sin_tab):
    half = vectors.shape[-1] // 2
    first = vectors[..., :half]
    second = vectors[..., half:]
    return jnp.concatenate([first * cos_tab - second * sin_tab, second * cos_tab + first * sin_tab], axis=-1)


def attend_sequence(item):
    q_seq, k_seq, v_seq, prefix = item
    key_pos = jnp.arange(SEQ_LEN)

    def one_block(block_item):
        q_rows, start = block_item
        row_pos = start + jnp.arange(ROW_BLOCK)
        visible = (key_pos[None, :] < prefix) | (key_pos[None, :] <= row_pos[:, None])
        scores = jnp.einsum('qhe,ke->hqk', q_rows, k_seq)
        scores = jnp.where(visible[None], scores, MASK_FILL)
        attn_probs = to_bf16_grid(jax.nn.softmax(scores, axis=-1))
        return to_bf16_grid(jnp.einsum('hqk,ke->qhe', attn_probs, v_seq))

    blocks = q_seq.reshape(SEQ_LEN // ROW_BLOCK, ROW_BLOCK, HEADS, HEAD_DIM)
    starts = jnp.arange(SEQ_LEN // ROW_BLOCK) * ROW_BLOCK
    attn_out = lax.map(jax.checkpoint(one_block), (blocks, starts))
    return attn_out.reshape(SEQ_LEN, HEADS, HEAD_DIM)


def block_forward(x, gain, w_q, w_k, w_v, w_o, prefix_len):
    x_f32 = x.astype(jnp.float32)
    inv_rms = lax.rsqrt(jnp.mean(x_f32 * x_f32, axis=-1, keepdims=True) + NORM_EPS)
    normed = to_bf16_grid(x_f32 * inv_rms * (1.0 + gain))
    cos_tab, sin_tab = rope_tables(jnp.arange(SEQ_LEN))
    q_proj = jnp.einsum('bsd,de->bse', normed, w_q).reshape(BATCH, SEQ_LEN, HEADS, HEAD_DIM)
    queries = to_bf16_grid(apply_rope(q_proj, cos_tab[:, None, :], sin_tab[:, None, :]) * HEAD_DIM ** -0.5)
    keys = to_bf16_grid(apply_rope(jnp.einsum('bsd,de->bse', normed, w_k), cos_tab, sin_tab))
    values = to_bf16_grid(jnp.einsum('bsd,de->bse', normed, w_v))
    attn_out = lax.map(attend_sequence, (queries, keys, values, prefix_len))
    mixed = jnp.einsum('bse,ed->bsd', attn_out.reshape(BATCH, SEQ_LEN, HEADS * HEAD_DIM), w_o)
    return (x_f32 + mixed).astype(jnp.bfloat16)


def reference(x, dy, prefix_len, w_norm, w_q, w_k, w_v, w_o):
    forward = functools.partial(block_forward, prefix_len=prefix_len)
    y_out, pull_back = jax.vjp(forward, x, w_norm.astype(jnp.float32), w_q.astype(jnp.float32), w_k.astype(jnp.float32), w_v.astype(jnp.float32), w_o.astype(jnp.float32))
    dx_out, d_gain, d_wq, d_wk, d_wv, d_wo = pull_back(dy)
    return y_out, dx_out, d_wq, d_wk, d_wv, d_wo, d_gain
```

```python
import functools
import jax
import jax.numpy as jnp
from jax import lax
from jax.experimental import pallas as pl
from jax.experimental.pallas import tpu as pltpu
from jax.sharding import PartitionSpec as P


ROPE_THETA = 10000.0
NORM_EPS = 1e-6
MASK_FILL = -1e30
HEAD_DIM = 256
HALF = HEAD_DIM // 2
SLOTS = 8
CORE, X, Y = 1, 2, 4
HEADS = 2
GROUPS = 8
PROJECTIONS = ((0,), (1,), (2, 3), (4, 5), (6, 7))
SPLIT = (2, 2, 1, 1, 1, 1, 1, 1)
PLACES = ((0, 1, 2, 3), (4, 5), (6,), (7,))
BF16 = jnp.bfloat16
F32 = jnp.float32
VMEM_LIMIT = 67_000_000


NT = (((1,), (1,)), ((), ()))
NN = (((1,), (0,)), ((), ()))
TN = (((0,), (0,)), ((), ()))
HBM = pl.BlockSpec(memory_space=pl.ANY)
shape = jax.ShapeDtypeStruct


def dot(a, b, dims):
    return lax.dot_general(a, b, dims, preferred_element_type=F32)


LOW, _ = range(2)


def whole_block(a):
    return pl.BlockSpec(a.shape, lambda *_: (0,) * len(a.shape))


def row_block(rows, cols, first=0):
    return pl.BlockSpec((rows, cols), lambda i, *_: (i + first, 0))


def col_block(rows, cols, first=0):
    return pl.BlockSpec((rows, cols), lambda i, *_: (0, i + first))


def cost(flops, moved, exps=0):
    return pl.CostEstimate(flops=flops, bytes_accessed=moved, transcendentals=exps)


def load(ref):
    return ref[...]


def params(**kw):
    return pltpu.CompilerParams(vmem_limit_bytes=VMEM_LIMIT, dimension_semantics=("arbitrary",), **kw)


def prepare_kernel(x_ref, gain, w_k, w_v, cos_ref, sin_ref, *refs):
    normed, inv_ref, kv = refs[-3:]
    x = load(x_ref).astype(F32)
    inv = lax.rsqrt(jnp.mean(x * x, axis=-1, keepdims=True) + NORM_EPS)
    inv_ref[...] = jnp.broadcast_to(inv, inv_ref.shape)
    xn = (x * inv * load(gain)).astype(BF16)
    normed[...] = xn
    k = dot(xn, load(w_k), NN)
    lo, hi = k[:, :HALF], k[:, HALF:]
    cos, sin = load(cos_ref), load(sin_ref)
    kv[0, :, :HALF] = (lo * cos - hi * sin).astype(BF16)
    kv[0, :, HALF:HEAD_DIM] = (hi * cos + lo * sin).astype(BF16)
    kv[0, :, HEAD_DIM:] = dot(xn, load(w_v), NN).astype(BF16)


def prepare(x, gain, w_k, w_v, cos, sin, batch0, count, old):
    tokens, width = x.shape
    seq = cos.shape[0]
    rows = row_block(seq, width, batch0)
    args = [x, gain, w_k, w_v, cos, sin]
    return pl.pallas_call(
        prepare_kernel,
        out_shape=[shape((tokens, width), BF16), shape((tokens, HALF), F32), shape((count, seq, 2 * HEAD_DIM), BF16)],
        grid=(count,),
        in_specs=[rows] + [whole_block(a) for a in args[1:]] + [HBM] * len(old),
        out_specs=[
            rows,
            row_block(seq, HALF, batch0),
            pl.BlockSpec((1, seq, 2 * HEAD_DIM), lambda b: (b, 0, 0)),
        ],
        input_output_aliases={len(args) + i: i for i in range(len(old))},
        compiler_params=params(),
        cost_estimate=cost(4 * count * seq * width * HEAD_DIM, 4 * count * seq * width),
        name="prepare",
    )(*args, *old)


def slot(s):
    return slice(s * HEAD_DIM, (s + 1) * HEAD_DIM)


def half_slot(s, k):
    return slice(s * HEAD_DIM + k * HALF, s * HEAD_DIM + (k + 1) * HALF)


def attention_kernel(mode, heads, batch0, key_sets, *refs):
    start, resume = mode
    it = iter(refs)
    meta, prefix = next(it), next(it)
    q_parts = [next(it), next(it)]
    do_parts = [next(it), next(it)]
    kv_in = [[next(it) for _ in range(SLOTS)] for _ in range(key_sets)]
    cos_ref, sin_ref = next(it), next(it)
    acc_in = [next(it) for _ in range(resume[0])]
    for _ in range(resume[1]):
        next(it)
    acc = [next(it) for _ in range(4)]
    o_all, dq_all = next(it), next(it)
    o_mine, dq_mine, others = next(it), next(it), next(it)
    qs, dos, limit, s_buf, dp_buf, p_buf = [next(it) for _ in range(6)]
    kv = kv_in[0]
    if key_sets == 2:
        kv = next(it)
        low = pl.program_id(0) < pl.num_programs(0) // 2

        @pl.when(low)
        def _():
            for s in range(SLOTS):
                kv[s] = kv_in[0][s][0]

        @pl.when(jnp.logical_not(low))
        def _():
            for s in range(SLOTS):
                kv[s] = kv_in[1][s][0]
    else:
        kv = [ref.at[0] for ref in kv_in[0]]
    seq = cos_ref.shape[0]
    rows = heads * seq
    half_heads = heads // 2
    me, core = meta[0], meta[1]
    cos, sin = cos_ref[...], sin_ref[...]
    scale = HEAD_DIM ** -0.5

    for part in range(2):
        for j in range(half_heads):
            r = (part * half_heads + j) * seq
            a = q_parts[part][:, half_slot(j, 0)]
            b = q_parts[part][:, half_slot(j, 1)]
            qs[r:r + seq, :HALF] = ((a * cos - b * sin) * scale).astype(BF16)
            qs[r:r + seq, HALF:] = ((b * cos + a * sin) * scale).astype(BF16)
            dos[r:r + seq, :] = do_parts[part][:, slot(j)]

    if key_sets == 2:
        keys = lambda s: kv[s, :, :HEAD_DIM]
        values = lambda s: kv[s, :, HEAD_DIM:]
    else:
        keys = lambda s: kv[s][:, :HEAD_DIM]
        values = lambda s: kv[s][:, HEAD_DIM:]
    row = lax.broadcasted_iota(jnp.int32, (seq, HALF), 0)
    limit[...] = jnp.maximum(row + (me * seq + 1), prefix[pl.program_id(0) + batch0])
    if start:
        for ref in acc:
            ref[...] = jnp.zeros(ref.shape, F32)
    else:
        for ref, old in zip(acc, acc_in):
            ref[...] = old[...]

    lane = lax.broadcasted_iota(jnp.int32, (seq, HALF), 1)
    bound = jnp.concatenate([limit[...]] * heads, axis=0)
    lanes = jnp.concatenate([lane] * heads, axis=0)
    q, do = qs[...], dos[...]

    top = jnp.full((rows, HALF), -jnp.inf, F32)
    for s in range(SLOTS):
        scores = dot(q, keys(s), NT)
        t = bound - lax.bitwise_xor(me, s) * seq
        left = jnp.where(lanes < t, scores[:, :HALF], MASK_FILL)
        right = jnp.where(lanes < t - HALF, scores[:, HALF:], MASK_FILL)
        top = jnp.maximum(top, jnp.maximum(left, right))
        s_buf[:, half_slot(s, 0)] = left
        s_buf[:, half_slot(s, 1)] = right
    top = jnp.broadcast_to(jnp.max(top, axis=1, keepdims=True), (rows, HALF))

    total = jnp.zeros((rows, HALF), F32)
    for s in range(SLOTS):
        for k in range(2):
            cols = half_slot(s, k)
            e = jnp.exp(s_buf[:, cols] - top)
            total = total + e
            s_buf[:, cols] = e
        dp = dot(do, values(s), NT)
        dp_buf[:, slot(s)] = dp.astype(BF16)
    inv = jnp.broadcast_to(1.0 / jnp.sum(total, axis=1, keepdims=True), (rows, HALF))

    delta = jnp.zeros((rows, HALF), F32)
    o = jnp.zeros((rows, HEAD_DIM), F32)
    for s in range(SLOTS):
        for k in range(2):
            cols = half_slot(s, k)
            p = s_buf[:, cols] * inv
            s_buf[:, cols] = p
            p_buf[:, cols] = p.astype(BF16)
            delta = delta + p * dp_buf[:, cols].astype(F32)
        p16 = p_buf[:, slot(s)]
        o = o + dot(p16, values(s), NN)
        acc[2 + s % 2][s // 2, 0] += dot(p16, do, TN)
    delta = jnp.broadcast_to(jnp.sum(delta, axis=1, keepdims=True), (rows, HALF))

    dq = jnp.zeros((rows, HEAD_DIM), F32)
    for s in range(SLOTS):
        for k in range(2):
            cols = half_slot(s, k)
            ds = s_buf[:, cols] * (dp_buf[:, cols].astype(F32) - delta)
            dp_buf[:, cols] = ds.astype(BF16)
        ds16 = dp_buf[:, slot(s)]
        dq = dq + dot(ds16, keys(s), NN)
        acc[s % 2][s // 2, 0] += dot(ds16, q, TN)
    qs[...] = dq.astype(BF16)
    dos[...] = o.astype(BF16)

    for part in range(2):
        for j in range(half_heads):
            r = (part * half_heads + j) * seq
            at = j * HEAD_DIM
            o_head = dos[r:r + seq, :]
            d = qs[r:r + seq, :].astype(F32) * scale
            a, b = d[:, :HALF], d[:, HALF:]
            d0 = (a * cos + b * sin).astype(BF16)
            d1 = (b * cos - a * sin).astype(BF16)
            o_to = o_mine if part == 0 else others.at[0]
            dq_to = dq_mine if part == 0 else others.at[1]
            o_to[at:at + HEAD_DIM, :] = jnp.transpose(o_head)
            dq_to[at:at + HALF, :] = jnp.transpose(d0)
            dq_to[at + HALF:at + HEAD_DIM, :] = jnp.transpose(d1)
            side = core if part == 0 else 1 - core
            at = pl.multiple_of(side * (half_heads * HEAD_DIM) + at, HEAD_DIM)
            o_all[:, pl.ds(at, HEAD_DIM)] = o_head
            dq_all[:, pl.ds(at, HALF)] = d0
            dq_all[:, pl.ds(pl.multiple_of(at + HALF, HALF), HALF)] = d1


def attention(meta, prefix, q, do, kvs, cos, sin, old, mode, q_block, group, batch0, count, width):
    tokens = q.shape[0]
    heads, cols = HEADS, HEADS * HEAD_DIM
    seq = cos.shape[0]
    batch = tokens // seq
    split = kvs[0][0].shape[0]
    key_sets = len(kvs)
    key0 = batch0 % split if key_sets == 1 else 0
    mine = pl.BlockSpec((seq, cols // 2), lambda b, meta, prefix: (b + batch0, 2 * q_block + meta[1]))
    other = pl.BlockSpec((seq, cols // 2), lambda b, meta, prefix: (b + batch0, 2 * q_block + 1 - meta[1]))
    if key_sets == 1:
        where = [lambda b, *_: (b + key0, 0, 0)]
    else:
        where = [lambda b, *_: (jnp.minimum(b, split - 1), 0, 0), lambda b, *_: (jnp.maximum(b - split, 0), 0, 0)]
    kv_specs = [pl.BlockSpec((1, seq, 2 * HEAD_DIM), w) for w in where for _ in range(SLOTS)]
    acc_spec = pl.BlockSpec((SLOTS // 2, 1, seq, HEAD_DIM), lambda b, *_: (0, b + batch0, 0, 0))
    part_spec = col_block(cols // 2, seq, batch0)
    others_spec = pl.BlockSpec((2, cols // 2, seq), lambda b, *_: (0, 0, b + batch0))
    all_spec = pl.BlockSpec((seq, cols), lambda b, *_: (b + batch0, group))
    in_specs = [mine, other, mine, other] + kv_specs + [whole_block(cos), whole_block(sin)]
    args = [q, q, do, do, *(kv for part in kvs for kv in part), cos, sin]
    alias = {}
    acc, every, parts = old
    read = not mode and acc is not None
    skipped = 0
    out_at = 0
    for arrays, size in ((acc, 4), (every, 2), (parts, 3)):
        if arrays is not None:
            for i, a in enumerate(arrays):
                alias[2 + len(args)] = out_at + i
                args.append(a)
            reads = read and out_at == 0
            in_specs += [acc_spec if reads else HBM] * size
            skipped += 0 if reads else size
        out_at += size
    rows = heads * seq
    keys = SLOTS * seq
    out = pl.pallas_call(
        functools.partial(attention_kernel, (mode, (4 if read else 0, skipped)), heads, batch0, key_sets),
        out_shape=[shape((SLOTS // 2, batch, seq, HEAD_DIM), F32)] * 4 + [shape((tokens, width), BF16)] * 2
        + [shape((cols // 2, tokens), BF16)] * 2 + [shape((2, cols // 2, tokens), BF16)],
        grid_spec=pltpu.PrefetchScalarGridSpec(
            num_scalar_prefetch=2,
            grid=(count,),
            in_specs=in_specs,
            out_specs=[acc_spec] * 4 + [all_spec] * 2 + [part_spec] * 2 + [others_spec],
            scratch_shapes=[
                pltpu.VMEM((rows, HEAD_DIM), BF16),
                pltpu.VMEM((rows, HEAD_DIM), BF16),
                pltpu.VMEM((seq, HALF), jnp.int32),
                pltpu.VMEM((rows, keys), F32),
                pltpu.VMEM((rows, keys), BF16),
                pltpu.VMEM((rows, keys), BF16),
            ] + ([pltpu.VMEM((SLOTS, seq, 2 * HEAD_DIM), BF16)] if key_sets == 2 else []),
        ),
        input_output_aliases=alias,
        compiler_params=params(),
        cost_estimate=cost(12 * rows * count * keys * HEAD_DIM, 8 * count * seq * cols + 16 * count * keys * HEAD_DIM,
            rows * count * keys),
        name="attention",
    )(meta, prefix, *args)
    return out[0:4], out[4:6], out[6:9]


def weight_grad_kernel(axis, meta, a_own, a_sib, b_own, b_sib, keep, send):
    rows = keep.shape[0]
    out = dot(load(a_own), load(b_own), NN) + dot(load(a_sib), load(b_sib), NN)

    @pl.when(meta[axis] == 0)
    def _():
        keep[...] = out[:rows]
        send[...] = out[rows:]

    @pl.when(meta[axis] != 0)
    def _():
        keep[...] = out[rows:]
        send[...] = out[:rows]


def weight_grad(meta, axis, a_own, a_sib, which, b_own, b_sib, col0=0, cols=None):
    width, tokens = a_own.shape
    tile = 1024 if width <= HEAD_DIM else 512
    cols = cols or b_own.shape[1]
    rows = width // 2
    sib_spec = pl.BlockSpec((None, width, tokens), lambda i, meta: (which, 0, 0))
    b_spec = col_block(tokens, tile, col0 // tile)
    out_spec = col_block(rows, tile)
    return pl.pallas_call(
        functools.partial(weight_grad_kernel, axis),
        out_shape=[shape((rows, cols), F32)] * 2,
        grid_spec=pltpu.PrefetchScalarGridSpec(
            num_scalar_prefetch=1,
            grid=(cols // tile,),
            in_specs=[whole_block(a_own), sib_spec, b_spec, b_spec],
            out_specs=[out_spec, out_spec],
        ),
        compiler_params=params(),
        cost_estimate=cost(8 * rows * tokens * cols, 4 * tokens * cols + 8 * rows * cols),
        name="weight_grad",
    )(meta, a_own, a_sib, b_own, b_sib)


def add_first_kernel(_, keep_a, got_a, keep_b, got_b, send_a, send_b):
    send_a[...] = load(keep_a) + load(got_a)
    send_b[...] = load(keep_b) + load(got_b)


def add_first(meta, keep_a, got_a, keep_b, got_b, steps=2):
    rows, cols = keep_a.shape
    half = (rows // 2, cols // steps)
    a = pl.BlockSpec(half, lambda i, meta: (1 - meta[3], i))
    b = pl.BlockSpec(half, lambda i, meta: (1 - meta[2], i))
    out = col_block(*half)
    return pl.pallas_call(
        add_first_kernel,
        out_shape=[shape((rows // 2, cols), F32)] * 2,
        grid_spec=pltpu.PrefetchScalarGridSpec(
            num_scalar_prefetch=1, grid=(steps,), in_specs=[a, a, b, b], out_specs=[out, out]),
        compiler_params=params(),
        cost_estimate=cost(rows * cols, 12 * rows * cols),
        name="add_first",
    )(meta, keep_a, got_a, keep_b, got_b)


def add_second_kernel(_, keep_a, got_a, last_a, keep_b, got_b, last_b, out):
    out[0] = load(keep_a) + load(got_a) + load(last_a)
    out[1] = load(keep_b) + load(got_b) + load(last_b)


def add_second(meta, keep_a, got_a, last_a, keep_b, got_b, last_b, steps=2):
    rows, cols = keep_a.shape
    half = (rows // 2, cols // steps)
    a = pl.BlockSpec(half, lambda i, meta: (meta[3], i))
    b = pl.BlockSpec(half, lambda i, meta: (meta[2], i))
    last = col_block(*half)
    return pl.pallas_call(
        add_second_kernel,
        out_shape=shape((2, rows // 2, cols), F32),
        grid_spec=pltpu.PrefetchScalarGridSpec(
            num_scalar_prefetch=1, grid=(steps,), in_specs=[a, a, last, b, b, last],
            out_specs=pl.BlockSpec((2,) + half, lambda i, meta: (0, 0, i))),
        compiler_params=params(),
        cost_estimate=cost(2 * rows * cols, 16 * rows * cols),
        name="add_second",
    )(meta, keep_a, got_a, last_a, keep_b, got_b, last_b)


def piece_order(order):
    bit = {X: 1, Y: 2}
    return [(m % 2) * 4 + ((m >> bit[order[0]]) & 1) * 2 + ((m >> bit[order[1]]) & 1) for m in range(SLOTS)]


def place_kernel(transposed, count, per, *refs):
    out = refs[-1]
    for g in range(count):
        a, b = refs[2 * g:2 * g + 2]

        @pl.when(pl.program_id(0) // per == g)
        def _():
            rows = jnp.concatenate([load(a), load(b)], axis=0)
            out[...] = jnp.transpose(rows) if transposed else rows


def place(which, groups, indices, into, out_shape):
    transposed = which == 1
    rows, cols = groups[0].shape
    size = rows // (2 * SLOTS)
    first = into is None
    per = SLOTS // 2
    hi, lo = (Y, X) if transposed else (X, Y)

    def source(g, part):
        def where(i):
            j = jnp.clip(i - g * per, 0, per - 1)
            return 2 * ((j >> 1) + (j & 1) * hi + part * lo) + which, 0

        return pl.BlockSpec((size, cols), where)

    def place_of(i):
        return sum(jnp.where(i // per == n, index, 0) for n, index in enumerate(indices)) * per + i % per

    if transposed:
        out_spec = pl.BlockSpec((cols, 2 * size), lambda i: (0, place_of(i)))
    else:
        out_spec = pl.BlockSpec((2 * size, cols), lambda i: (place_of(i), 0))
    specs = [source(g, part) for g in range(len(groups)) for part in range(2)]
    args = [g for g in groups for _ in range(2)]
    return pl.pallas_call(
        functools.partial(place_kernel, transposed, len(groups), per),
        out_shape=shape(out_shape, F32),
        grid=(per * len(groups),),
        in_specs=specs + ([] if first else [HBM]),
        out_specs=out_spec,
        input_output_aliases={} if first else {len(args): 0},
        compiler_params=params(),
        cost_estimate=cost(len(groups) * rows * cols // 2, len(groups) * 4 * rows * cols),
        name="place",
    )(*args, *([] if first else [into]))


def place_kv_kernel(steps, orders, src, w_k, w_v, buf):
    size = src.shape[1]
    for which, order in enumerate(orders):
        @pl.when(pl.program_id(0) // steps == which)
        def _():
            for m, at in enumerate(order):
                buf[at * size:(at + 1) * size, :] = src[m]

    w_k[...] = jnp.transpose(buf[:HEAD_DIM])
    w_v[...] = jnp.transpose(buf[HEAD_DIM:])


def place_kv(gathered, tile=512):
    rows, cols = gathered.shape
    steps = cols // tile
    size = rows // (2 * SLOTS)
    out_spec = row_block(tile, HEAD_DIM)
    return pl.pallas_call(
        functools.partial(place_kv_kernel, steps, [piece_order(o) for o in ((X, Y), (Y, X))]),
        out_shape=[shape((2 * cols, HEAD_DIM), F32)] * 2,
        grid=(2 * steps,),
        in_specs=[pl.BlockSpec((SLOTS, None, size, tile), lambda i: (0, i // steps, 0, i % steps))],
        out_specs=[out_spec, out_spec],
        scratch_shapes=[pltpu.VMEM((2 * HEAD_DIM, tile), F32)],
        compiler_params=params(),
        cost_estimate=cost(rows * cols, 8 * rows * cols),
        name="place_kv",
    )(gathered.reshape(SLOTS, 2, size, cols))


def norm_grad_kernel(part, dk, dv, w_k, w_v, x_ref, dy, inv_ref, gain, dx, d_gain):
    total = load(part) + dot(load(dk), load(w_k), NT) + dot(load(dv), load(w_v), NT)
    d_normed = total.astype(BF16).astype(F32)
    inv = inv_ref[:, 0:1]
    scaled = load(x_ref).astype(F32) * inv
    grad = jnp.sum(d_normed * scaled, axis=0, keepdims=True)

    @pl.when(pl.program_id(0) == 0)
    def _():
        d_gain[...] = jnp.zeros(d_gain.shape, F32)

    d_gain[0:1, :] += grad
    u = d_normed * load(gain)
    back = inv * (u - scaled * jnp.mean(u * scaled, axis=-1, keepdims=True))
    dx[...] = (load(dy).astype(F32) + back).astype(BF16)


def norm_grad(part, dk, dv, w_k, w_v, x, dy, inv, gain, tile=256):
    tokens, width = x.shape
    rows, head = row_block(tile, width), row_block(tile, HEAD_DIM)
    weight = whole_block(w_k)
    dx, d_gain = pl.pallas_call(
        norm_grad_kernel,
        out_shape=[shape((tokens, width), BF16), shape((8, width), F32)],
        grid=(tokens // tile,),
        in_specs=[rows, head, head, weight, weight, rows, rows, row_block(tile, HALF), whole_block(gain)],
        out_specs=[rows, pl.BlockSpec((8, width), lambda i: (0, 0))],
        compiler_params=params(),
        cost_estimate=cost(4 * tokens * width * HEAD_DIM, 10 * tokens * width),
        name="norm_grad",
    )(part, dk, dv, w_k, w_v, x, dy, inv, gain)
    return dx, d_gain[0]


def swap(value, mask):
    return lax.ppermute(value, 'sp', [(i, i ^ mask) for i in range(SLOTS)])


def gather(value):
    return lax.all_gather(value, 'sp', axis=0, tiled=True)


def solution(mesh):
    seq_spec = P(None, 'sp', None)
    whole = P()

    def block(x, dy, prefix_len, w_norm, w_q, w_k, w_v, w_o):
        batch, seq, d_model = x.shape
        split = batch // 2
        tokens = batch * seq
        width = w_q.shape[1]
        me = lax.axis_index('sp').astype(jnp.int32)
        bits = [me & 1, (me >> 1) & 1, me >> 2]
        meta = jnp.stack([me, *bits])
        x = x.reshape(tokens, d_model)
        dy = dy.reshape(tokens, d_model)
        dy_sib = swap(dy, CORE)

        frequencies = ROPE_THETA ** (-2.0 * jnp.arange(HALF, dtype=F32) / HEAD_DIM)
        angles = (me * seq + jnp.arange(seq)).astype(F32)[:, None] * frequencies[None, :]
        cos, sin = jnp.cos(angles), jnp.sin(angles)
        gain = (1.0 + w_norm.astype(F32))[None, :]

        def keys_of_all(own):
            kvs = [None] * SLOTS
            kvs[0] = own
            for mask in (X, Y, X | Y):
                kvs[mask] = swap(own, mask)
            for slot in (0, X, Y, X | Y):
                kvs[slot + 1] = swap(kvs[slot], CORE)
            return kvs

        normed, inv_rms, kv_low = prepare(x, gain, w_k, w_v, cos, sin, LOW, split, ())
        kvs_low = keys_of_all(kv_low)
        normed, inv_rms, kv_high = prepare(x, gain, w_k, w_v, cos, sin, split, split, (normed, inv_rms))
        kvs_high = keys_of_all(kv_high)
        normed_sib = swap(normed, CORE)

        def sum_over_chips(a, b):
            got_a = swap(a[1], X)
            got_b = swap(b[1], Y)
            send_a, send_b = add_first(meta, a[0], got_a, b[0], got_b)
            last_a = swap(send_a, Y)
            last_b = swap(send_b, X)
            done = add_second(meta, a[0], got_a, last_a, b[0], got_b, last_b)
            return gather(done.reshape(-1, done.shape[-1]))

        projected = {}
        for groups in PROJECTIONS:
            c0, c1 = (g * HEADS * HEAD_DIM for g in (groups[0], groups[-1] + 1))
            q = dot(normed, w_q[:, c0:c1], NN)
            do = dot(dy, w_o[c0:c1, :], NT).astype(BF16)
            for g in groups:
                projected[g] = (q, do, g - groups[0])

        acc = every = None
        gathered = []
        for g in range(GROUPS):
            q, do, q_block = projected[g]
            parts = None
            for part in range(SPLIT[g]):
                batch0, count = part * batch // SPLIT[g], batch // SPLIT[g]
                if SPLIT[g] == 1:
                    kvs = [kvs_low, kvs_high]
                else:
                    kvs = [kvs_low if batch0 < split else kvs_high]
                acc, every, parts = attention(
                    meta, prefix_len, q, do, kvs, cos, sin, (acc, every, parts), g == 0,
                    q_block, g, batch0, count, width)
            o_mine, dq_mine, others = parts
            sib = swap(others, CORE)
            o_rows = weight_grad(meta, 2, o_mine, sib, 0, dy, dy_sib)
            q_rows = weight_grad(meta, 3, dq_mine, sib, 1, normed, normed_sib)
            gathered.append(sum_over_chips(o_rows, q_rows))
        o_all, dq_all = every

        def kv_sum(even, odd, order):
            got = swap(odd, CORE)
            first, second = order
            near = second // 2
            if first == X:
                out = even[1::2] + got[1::2]
            else:
                out = even[2:] + got[2:]
            got1 = swap(out, first)
            out2 = even[near] + got[near] + got1[1]
            got2 = swap(out2, second)
            return (even[0] + got[0] + got1[0] + got2).astype(BF16)

        dk_own = kv_sum(acc[0], acc[1], (X, Y))
        dv_own = kv_sum(acc[2], acc[3], (Y, X)).reshape(tokens, HEAD_DIM)
        d = dk_own.astype(F32)
        a, b = d[..., :HALF], d[..., HALF:]
        dk_proj = jnp.concatenate([a * cos + b * sin, b * cos - a * sin], axis=-1).astype(BF16).reshape(tokens, HEAD_DIM)

        turned_k, turned_v = dk_proj.T, dv_own.T
        a_own = jnp.where(bits[0] == 0, turned_k, turned_v)
        a_out = jnp.where(bits[0] == 0, turned_v, turned_k)
        a_sib = swap(a_out, CORE)[None]
        half = d_model // 2
        left = weight_grad(meta, 2, a_own, a_sib, 0, normed, normed_sib, 0, half)
        right = weight_grad(meta, 3, a_own, a_sib, 0, normed, normed_sib, half, half)
        kv_rows = sum_over_chips(left, right)

        y = (x.astype(F32) + dot(o_all, w_o, NN)).astype(BF16).reshape(batch, seq, d_model)
        part = dot(dq_all, w_q, NT)
        dx, d_gain = norm_grad(part, dk_proj, dv_own, w_k, w_v, x, dy, inv_rms, gain)
        dx = dx.reshape(batch, seq, d_model)
        for mask in (CORE, X, Y):
            got = swap(d_gain, mask)
            d_gain = d_gain + got

        d_wo = d_wq = None
        for groups in PLACES:
            rows_in = [gathered[g] for g in groups]
            d_wo = place(0, rows_in, groups, d_wo, w_o.shape)
            d_wq = place(1, rows_in, groups, d_wq, w_q.shape)
        d_wk, d_wv = place_kv(kv_rows)
        return y, dx, d_wq, d_wk, d_wv, d_wo, d_gain

    return jax.shard_map(block, mesh=mesh, in_specs=(seq_spec, seq_spec, whole, whole, whole, whole, whole, whole), out_specs=(seq_spec, seq_spec, whole, whole, whole, whole, whole), check_vma=False)
```
